32 devices in a mesh: local: 4 (over y, x), dp: 8 (over z, core).
Axes of the slice: x: 2, y: 2, z: 4, core: 2. Of those that a mesh axis runs over, the one named last changes fastest.
Arguments:
- gradient: bfloat16 [32, 72, 7168], P(('local', 'dp')), may hold values from -1.1953125 to 1.1953125
- feedback: bfloat16 [32, 72, 7168], P(('local', 'dp')), may hold values from -0.59765625 to 0.59765625
- basis_in: float32 [7168, 32], replicated, may hold values from -6 to 6
Outputs:
- new_feedback: bfloat16 [32, 72, 7168], P(('local', 'dp'))
- new_basis: float32 [7168, 32], replicated
The draws below stay inside these ranges and needn't reach their ends.
All inputs are finite; a program needn't handle non-finite values.
Results may differ from the reference program's by a relative error of at most 0.001.
Values sent between devices are 32-bit elements; how exact they have to be, the bound alone decides.
No kernel may reach another device: no remote copies, remote signals or barrier semaphores. Data moves between devices by JAX's collectives and lax.ppermute only.
A program may use at most 64 MiB of HBM per device.

```python
import jax
import jax.numpy as jnp
from jax import lax

ROWS = 72
FF = 7168
RANK = 32
WORKERS = 32


def level_of(rng, dims, split, least, largest):
    gain = 1.0
    for position, shards_of in split:
        draws = jax.random.uniform(jax.random.fold_in(jax.random.fold_in(rng, 6), position), (shards_of,), jnp.float32, least / len(split), largest / len(split))
        gain = gain * jnp.repeat(jnp.exp(draws), dims[position] // shards_of).reshape((-1,) + (1,) * (len(dims) - 1 - position))
    return gain


def gaussian(own_key, extent, scale, limit, cuts=(), kind=jnp.bfloat16):
    factor_of = level_of(own_key, extent, cuts, -0.22, 0.18) if cuts else 1.0
    array = jax.random.normal(own_key, extent, jnp.float32) * scale * factor_of
    return jnp.minimum(jnp.maximum(array, -limit), limit).astype(kind)


def setup_inputs(seed: int = 0) -> dict:
    arg_keys = jax.random.split(jax.random.key(seed), 4)
    return {
        "gradient": gaussian(arg_keys[0], (WORKERS, ROWS, FF), 0.2, 1.1953125, ((0, 32),)),
        "feedback": gaussian(arg_keys[1], (WORKERS, ROWS, FF), 0.1, 0.59765625, ((0, 32),)),
        "basis_in": gaussian(arg_keys[2], (FF, RANK), 1.0, 6.0, (), jnp.float32),
    }


epsilon = 1e-06

def orthonormal(matrix):
    columns = []
    for column in range(matrix.shape[1]):
        vector = matrix[:, column]
        for earlier in columns:
            vector = vector - jnp.sum(earlier * vector) * earlier
        vector = vector * lax.rsqrt(jnp.sum(vector * vector) + epsilon)
        columns.append(vector)
    return jnp.stack(columns, axis=1)

def reference(gradient, feedback, basis_in):
    highest = lax.Precision.HIGHEST
    indices = jnp.arange(WORKERS, dtype=jnp.int32)

    def merged_of(index):
        return gradient[index].astype(jnp.float32) + feedback[index].astype(jnp.float32)

    def add_left(carry, index):
        return (carry + jnp.dot(merged_of(index), basis_in, precision=highest), None)
    left_sum, unused = lax.scan(add_left, jnp.zeros((ROWS, RANK), jnp.float32), indices)
    left_basis = orthonormal(left_sum)

    def add_right(carry, index):
        return (carry + jnp.dot(merged_of(index).T, left_basis, precision=highest), None)
    new_basis, unused = lax.scan(add_right, jnp.zeros((FF, RANK), jnp.float32), indices)
    approx = jnp.dot(left_basis, new_basis.T, precision=highest) / WORKERS

    def corrected(index):
        return (merged_of(index) - approx).astype(jnp.bfloat16)
    new_feedback = lax.map(corrected, indices)
    return (new_feedback, new_basis)
```

```python
import functools

import jax
import jax.numpy as jnp
from jax import lax
from jax.experimental import pallas as pl
from jax.experimental.pallas import tpu as pltpu
from jax.sharding import PartitionSpec as P

epsilon = 1e-06
AXES = ("local", "dp")
F32, BF16 = jnp.float32, jnp.bfloat16
VMEM = pltpu.VMEM


def call(kernel, outs, *args, flops=1 << 20, limit=12, scratch=()):
    spec = pl.BlockSpec(memory_space=VMEM)
    many = isinstance(outs, list)
    shapes = [jax.ShapeDtypeStruct(s, d) for s, d in (outs if many else [outs])]
    size = sum(a.size * a.dtype.itemsize for a in args)
    result = pl.pallas_call(
        kernel,
        out_shape=shapes,
        in_specs=[spec] * len(args),
        out_specs=[spec] * len(shapes),
        scratch_shapes=scratch,
        compiler_params=pltpu.CompilerParams(vmem_limit_bytes=limit << 20),
        cost_estimate=pl.CostEstimate(flops=flops, bytes_accessed=size, transcendentals=0),
    )(*args)
    return result if many else result[0]


def split(value):
    high = value.astype(BF16)
    return high, (value - high.astype(F32)).astype(BF16)


def send_kernel(g, f, out):
    half = out.shape[1]
    other = 1 - lax.rem(lax.axis_index("dp"), 2)
    span = pl.ds(pl.multiple_of(other * half, 128), half)
    out[...] = g[:, span].astype(F32) + f[:, span].astype(F32)


def left_kernel(g, f, b, out):
    rank = b.shape[0]
    high, low = split(b[...])
    pieces = jnp.concatenate([high, low], axis=0)
    dims = (((1,), (1,)), ((), ()))
    both = lax.dot_general(pieces, g[...], dims, preferred_element_type=F32)
    both += lax.dot_general(pieces, f[...], dims, preferred_element_type=F32)
    out[...] = both[:rank] + both[rank:]


def pair_kernel(g, f, got, *outs):
    width = outs[0].shape[1]
    half = got.shape[1]
    core = lax.rem(lax.axis_index("dp"), 2)
    mine = lax.axis_index("local")
    for step, out in enumerate(outs):
        chunk = partner(mine, step, len(outs))
        inner = pl.ds(pl.multiple_of(chunk * width, 128), width)
        span = pl.ds(pl.multiple_of(core * half + chunk * width, 128), width)
        out[...] = g[:, span].astype(F32) + f[:, span].astype(F32) + got[:, inner]


def partner(index, step, size):
    if size & (size - 1):
        return lax.rem(index + step, size)
    return jnp.bitwise_xor(index, step)


def gram_schmidt_kernel(block, a, b, basis, basis_t):
    rank, rows = a.shape
    lanes = 128
    total = jnp.concatenate([a[...] + b[...], jnp.zeros((lanes - rank, rows), F32)], axis=0)
    work = total.T
    lane = lax.broadcasted_iota(jnp.int32, (rows, lanes), 1)
    done = jnp.zeros((rows, lanes), F32)
    for start in range(0, rank, block):
        count = min(block, rank - start)
        columns = [jnp.broadcast_to(work[:, start + i : start + i + 1], (rows, lanes)) for i in range(count)]
        for i in range(count):
            column = columns[i]
            scale = lax.rsqrt(jnp.sum(column * column, axis=0, keepdims=True) + epsilon)
            unit = column * scale
            for k in range(i + 1, count):
                dot = jnp.sum(column * columns[k], axis=0, keepdims=True) * scale
                columns[k] = columns[k] - unit * dot
            dots = jnp.sum(column * work, axis=0, keepdims=True) * scale
            work = work - unit * dots
            done = jnp.where(lane == start + i, unit, done)
    basis[...] = done[:, :rank]
    basis_t[...] = done.T[:rank]


def right_kernel(basis_t, *refs):
    *terms, out = refs
    total = terms[0][...]
    for term in terms[1:]:
        total = total + term[...]
    out[...] = jnp.dot(basis_t[...], total, precision=lax.Precision.HIGHEST, preferred_element_type=F32)


def final_kernel(workers, g, f, basis, own, other, feedback, new_basis_t):
    chunks, rank, width = own.shape
    core = lax.rem(lax.axis_index("dp"), 2)
    high, low = split(basis[...] * (1.0 / workers))
    left = jnp.concatenate([high, low, high], axis=1)

    for part in range(2 * chunks):
        mine = core == part // chunks
        piece = jnp.where(mine, own[part % chunks], other[part % chunks])
        span = pl.ds(part * width, width)
        new_basis_t[:, span] = piece
        upper, lower = split(piece)
        right = jnp.concatenate([upper, upper, lower], axis=0)
        approx = jnp.dot(left, right, preferred_element_type=F32)
        feedback[:, span] = (g[:, span].astype(F32) + f[:, span].astype(F32) - approx).astype(BF16)


def body(gradient, feedback, basis_in):
    g, f = gradient[0], feedback[0]
    rows, columns = g.shape
    basis_t_in = basis_in.T
    rank = basis_t_in.shape[0]
    local, dp = lax.axis_size("local"), lax.axis_size("dp")
    groups = dp // 2
    half = columns // 2
    width = half // local

    def swap(value, axis, step, size, stride=1):
        pairs = []
        for source in range(lax.axis_size(axis)):
            place = source // stride % size
            if size & (size - 1):
                to = (place - step) % size
            else:
                to = place ^ step
            pairs.append((source, source + (to - place) * stride))
        return lax.ppermute(value, axis, pairs)

    def total_over(value, axis, size, stride):
        other = jnp.zeros_like(value)
        step = 1
        first = True
        while step < size:
            value = value if first else value + other
            other = swap(value, axis, step, size, stride)
            first = False
            step *= 2
        return value, other

    outgoing = call(send_kernel, ((rows, half), F32), g, f)
    got = swap(outgoing, "dp", 1, 2)
    left = call(left_kernel, ((rank, rows), F32), g, f, basis_t_in, flops=1 << 28)
    a, b = total_over(left, "local", local, 1)
    left = a + b
    got, left = lax.optimization_barrier((got, left))
    chunks = call(pair_kernel, [((rows, width), F32)] * local, g, f, got)
    terms = [chunks[0]] + [swap(chunks[s], "local", s, local) for s in range(1, local)]
    a, b = total_over(left, "dp", groups, 2)
    left = a + b
    a, b = left, swap(left, "dp", 1, 2)
    basis, basis_t = call(
        functools.partial(gram_schmidt_kernel, 4), [((rows, rank), F32), ((rank, rows), F32)], a, b, flops=1 << 24
    )
    right = call(right_kernel, ((rank, width), F32), basis_t, *terms)
    a, b = total_over(right, "dp", groups, 2)
    right = a + b
    own = lax.all_gather(right, "local", axis=0)
    other = swap(own, "dp", 1, 2)
    new_feedback, new_basis_t = call(
        functools.partial(final_kernel, local * dp),
        [((rows, columns), BF16), ((rank, columns), F32)],
        g, f, basis, own, other,
    )
    return (new_feedback[None], new_basis_t.T)


def solution(mesh):
    return jax.shard_map(
        body,
        mesh=mesh,
        in_specs=(P(("local", "dp"), None, None), P(("local", "dp"), None, None), P()),
        out_specs=(P(("local", "dp"), None, None), P()),
        check_vma=False,
    )
```

```python
import functools

import jax
import jax.numpy as jnp
from jax import lax
from jax.experimental import pallas as pl
from jax.experimental.pallas import tpu as pltpu
from jax.sharding import PartitionSpec as P


epsilon = 1e-06
AXES = ("local", "dp")
F32, BF16 = jnp.float32, jnp.bfloat16
VMEM = pltpu.VMEM
PIECES = 4


def call(kernel, outs, *args, flops=1 << 20, limit=12, scratch=(), space=VMEM):
    many = isinstance(outs, list)
    shapes = [jax.ShapeDtypeStruct(s, d) for s, d in (outs if many else [outs])]
    size = sum(a.size * a.dtype.itemsize for a in args)
    result = pl.pallas_call(
        kernel,
        out_shape=shapes,
        in_specs=[pl.BlockSpec(memory_space=space)] * len(args),
        out_specs=[pl.BlockSpec(memory_space=VMEM)] * len(shapes),
        scratch_shapes=scratch,
        compiler_params=pltpu.CompilerParams(vmem_limit_bytes=limit << 20),
        cost_estimate=pl.CostEstimate(flops=flops, bytes_accessed=size, transcendentals=0),
    )(*args)
    return result if many else result[0]


def split(value):
    high = value.astype(BF16)
    return high, (value - high.astype(F32)).astype(BF16)


def partner(index, step, size):
    if size & (size - 1):
        return (index + step) % size
    return index ^ step


def odd_bits(index, size):
    total = 0
    while size > 1 and not size & (size - 1):
        total, index, size = total + index % 2, index // 2, size // 2
    return total % 2


def own_half():
    local, dp = lax.axis_size("local"), lax.axis_size("dp")
    place = lax.axis_index("dp")
    return (place % 2 + odd_bits(lax.axis_index("local"), local) + odd_bits(place // 2, dp // 2)) % 2


def left_kernel(g, f, b, left, merged, send, gv, fv, bv, sems):
    rank = b.shape[0]
    pieces = sems.shape[1]
    width = g.shape[1] // pieces
    half = own_half()
    spans, copies = [], []
    for i in range(pieces):
        piece = (half * (pieces // 2) + i + pieces // 2) % pieces
        span = pl.ds(pl.multiple_of(piece * width, 128), width)
        spans.append(span)
        for j, (source, target) in enumerate(((g, gv), (f, fv), (b, bv))):
            copy = pltpu.make_async_copy(source.at[:, span], target.at[:, span], sems.at[j, i])
            copy.start()
            copies.append(copy)
    dims = (((1,), (1,)), ((), ()))
    total = None
    for i, span in enumerate(spans):
        for copy in copies[3 * i : 3 * i + 3]:
            copy.wait()
        high, low = split(bv[:, span])
        basis = jnp.concatenate([high, low], axis=0)
        one, two = gv[:, span], fv[:, span]
        part = lax.dot_general(basis, one, dims, preferred_element_type=F32)
        part += lax.dot_general(basis, two, dims, preferred_element_type=F32)
        total = part if total is None else total + part
        both = one.astype(F32) + two.astype(F32)
        merged[:, span] = both
        if i < pieces // 2:
            send[:, i * width : (i + 1) * width] = both
    left[...] = total[:rank] + total[rank:]


def pair_kernel(merged, got, *outs):
    width = outs[0].shape[1]
    mine = lax.axis_index("local")
    start = own_half() * got.shape[1]
    for step, out in enumerate(outs):
        inner = pl.multiple_of(partner(mine, step, len(outs)) * width, 128)
        span = pl.ds(pl.multiple_of(start + inner, 128), width)
        out[...] = merged[:, span] + got[:, pl.ds(inner, width)]


def gram_schmidt_kernel(block, a, b, basis, basis_t):
    rank, rows = a.shape
    lanes = 128
    total = jnp.concatenate([a[...] + b[...], jnp.zeros((lanes - rank, rows), F32)], axis=0)
    work = total.T
    lane = lax.broadcasted_iota(jnp.int32, (rows, lanes), 1)
    done = jnp.zeros((rows, lanes), F32)
    for start in range(0, rank, block):
        count = min(block, rank - start)
        columns = [jnp.broadcast_to(work[:, start + i : start + i + 1], (rows, lanes)) for i in range(count)]
        for i in range(count):
            column = columns[i]
            scale = lax.rsqrt(jnp.sum(column * column, axis=0, keepdims=True) + epsilon)
            unit = column * scale
            for k in range(i + 1, count):
                dot = jnp.sum(column * columns[k], axis=0, keepdims=True) * scale
                columns[k] = columns[k] - unit * dot
            dots = jnp.sum(column * work, axis=0, keepdims=True) * scale
            work = work - unit * dots
            done = jnp.where(lane == start + i, unit, done)
    basis[...] = done[:, :rank]
    basis_t[...] = done.T[:rank]


def right_kernel(basis_t, *refs):
    *terms, out = refs
    total = terms[0][...]
    for term in terms[1:]:
        total = total + term[...]
    out[...] = jnp.dot(basis_t[...], total, precision=lax.Precision.HIGHEST, preferred_element_type=F32)


def final_kernel(workers, merged, basis, *refs):
    *blocks, feedback, new_basis_t = refs
    chunks = len(blocks) // 2
    width = blocks[0].shape[1]
    mine = lax.axis_index("local")
    half = own_half()
    high, low = split(basis[...] * (1.0 / workers))
    left = jnp.concatenate([high, low, high], axis=1)
    for i, block in enumerate(blocks):
        side = half if i < chunks else 1 - half
        start = (side * chunks + partner(mine, i % chunks, chunks)) * width
        span = pl.ds(pl.multiple_of(start, 128), width)
        piece = block[...]
        new_basis_t[:, span] = piece
        upper, lower = split(piece)
        right = jnp.concatenate([upper, upper, lower], axis=0)
        approx = jnp.dot(left, right, preferred_element_type=F32)
        feedback[:, span] = (merged[:, span] - approx).astype(BF16)


def body(gradient, feedback, basis_in):
    g, f = gradient[0], feedback[0]
    rows, columns = g.shape
    b = basis_in.T
    rank = b.shape[0]
    local, dp = lax.axis_size("local"), lax.axis_size("dp")
    groups = dp // 2
    half = columns // 2
    width = half // local

    def permute(value, along_local, step):
        pairs = []
        for x in range(local):
            for z in range(groups):
                to = (partner(x, step, local), z) if along_local else (x, partner(z, step, groups))
                flip = odd_bits(step, local if along_local else groups)
                for core in range(2):
                    pairs.append((x * dp + 2 * z + core, to[0] * dp + 2 * to[1] + (core ^ flip)))
        if partner(0, step, local if along_local else groups) != step:
            pairs = [(to, source) for source, to in pairs]
        return lax.ppermute(value, AXES, pairs)

    def swap(value):
        return lax.ppermute(value, AXES, [(i, i ^ 1) for i in range(local * dp)])

    def total_over(value, along_local):
        size = local if along_local else groups
        double = not size & (size - 1)
        first = value
        step = 1
        while step < size:
            other = permute(value if double else first, along_local, step)
            value = value + other
            step = 2 * step if double else step + 1
        return value

    pieces = PIECES if columns % (128 * PIECES) == 0 else 2
    g, f, b = (pltpu.with_memory_space_constraint(x, pltpu.HBM) for x in (g, f, b))
    left, merged, send = call(
        left_kernel, [((rank, rows), F32), ((rows, columns), F32), ((rows, half), F32)],
        g, f, b, flops=1 << 27, limit=16,
        scratch=[VMEM(g.shape, g.dtype), VMEM(f.shape, f.dtype), VMEM(b.shape, b.dtype),
                 pltpu.SemaphoreType.DMA((3, pieces))],
        space=pltpu.HBM,
    )
    got = swap(send)
    left = total_over(left, True)
    chunks = call(pair_kernel, [((rows, width), F32)] * local, merged, got)
    terms = [chunks[0]] + [permute(chunks[s], True, s) for s in range(1, local)]
    left = total_over(left, False)
    basis, basis_t = call(
        functools.partial(gram_schmidt_kernel, 4),
        [((rows, rank), F32), ((rank, rows), F32)],
        left, swap(left), flops=1 << 26,
    )
    right = call(right_kernel, ((rank, width), F32), basis_t, *terms, flops=1 << 25)
    own = total_over(right, False)
    blocks = [own] + [permute(own, True, s) for s in range(1, local)]
    blocks += [swap(block) for block in blocks]
    new_feedback, new_basis_t = call(
        functools.partial(final_kernel, local * dp),
        [((rows, columns), BF16), ((rank, columns), F32)],
        merged, basis, *blocks, flops=1 << 27, limit=16,
    )
    return (new_feedback[None], new_basis_t.T)


def solution(mesh):
    return jax.shard_map(
        body,
        mesh=mesh,
        in_specs=(P(("local", "dp"), None, None), P(("local", "dp"), None, None), P()),
        out_specs=(P(("local", "dp"), None, None), P()),
        check_vma=False,
    )
```

```python
import functools

import jax
import jax.numpy as jnp
from jax import lax
from jax.experimental import pallas as pl
from jax.experimental.pallas import tpu as pltpu
from jax.sharding import PartitionSpec as P


epsilon = 1e-06
AXES = ("local", "dp")
F32, BF16 = jnp.float32, jnp.bfloat16
VMEM = pltpu.VMEM
PIECES = 4
PARTS = 2


def call(kernel, outs, *args, flops=1 << 20, limit=12, scratch=(), space=VMEM):
    many = isinstance(outs, list)
    shapes = [jax.ShapeDtypeStruct(s, d) for s, d in (outs if many else [outs])]
    size = sum(a.size * a.dtype.itemsize for a in args)
    result = pl.pallas_call(
        kernel,
        out_shape=shapes,
        in_specs=[pl.BlockSpec(memory_space=space)] * len(args),
        out_specs=[pl.BlockSpec(memory_space=VMEM)] * len(shapes),
        scratch_shapes=scratch,
        compiler_params=pltpu.CompilerParams(vmem_limit_bytes=limit << 20),
        cost_estimate=pl.CostEstimate(flops=flops, bytes_accessed=size, transcendentals=0),
    )(*args)
    return result if many else result[0]


def split(value):
    high = value.astype(BF16)
    return high, (value - high.astype(F32)).astype(BF16)


def partner(index, step, size):
    if size & (size - 1):
        return (index + step) % size
    return index ^ step


def odd_bits(index, size):
    total = 0
    while size > 1 and not size & (size - 1):
        total, index, size = total + index % 2, index // 2, size // 2
    return total % 2


def own_half():
    local, dp = lax.axis_size("local"), lax.axis_size("dp")
    place = lax.axis_index("dp")
    return (place % 2 + odd_bits(lax.axis_index("local"), local) + odd_bits(place // 2, dp // 2)) % 2


def left_kernel(g, f, b, left, merged, send, gv, fv, bv, sems):
    rank = b.shape[0]
    pieces = sems.shape[1]
    width = g.shape[1] // pieces
    half = own_half()
    spans, copies = [], []
    for i in range(pieces):
        piece = (half * (pieces // 2) + i + pieces // 2) % pieces
        span = pl.ds(pl.multiple_of(piece * width, 128), width)
        spans.append(span)
        for j, (source, target) in enumerate(((g, gv), (f, fv), (b, bv))):
            copy = pltpu.make_async_copy(source.at[:, span], target.at[:, span], sems.at[j, i])
            copy.start()
            copies.append(copy)
    dims = (((1,), (1,)), ((), ()))
    total = None
    for i, span in enumerate(spans):
        for copy in copies[3 * i : 3 * i + 3]:
            copy.wait()
        high, low = split(bv[:, span])
        basis = jnp.concatenate([high, low], axis=0)
        one, two = gv[:, span], fv[:, span]
        part = lax.dot_general(basis, one, dims, preferred_element_type=F32)
        part += lax.dot_general(basis, two, dims, preferred_element_type=F32)
        total = part if total is None else total + part
        both = one.astype(F32) + two.astype(F32)
        merged[:, span] = both
        if i < pieces // 2:
            send[:, i * width : (i + 1) * width] = both
    left[...] = total[:rank] + total[rank:]


def pair_kernel(merged, got, *outs):
    width = outs[0].shape[1]
    mine = lax.axis_index("local")
    start = own_half() * got.shape[1]
    for step, out in enumerate(outs):
        inner = pl.multiple_of(partner(mine, step, len(outs)) * width, 128)
        span = pl.ds(pl.multiple_of(start + inner, 128), width)
        out[...] = merged[:, span] + got[:, pl.ds(inner, width)]


def gram_schmidt_kernel(block, a, b, basis, basis_t):
    rank, rows = a.shape
    lanes = 128
    total = jnp.concatenate([a[...] + b[...], jnp.zeros((lanes - rank, rows), F32)], axis=0)
    work = total.T
    lane = lax.broadcasted_iota(jnp.int32, (rows, lanes), 1)
    done = jnp.zeros((rows, lanes), F32)
    for start in range(0, rank, block):
        count = min(block, rank - start)
        columns = [jnp.broadcast_to(work[:, start + i : start + i + 1], (rows, lanes)) for i in range(count)]
        for i in range(count):
            column = columns[i]
            scale = lax.rsqrt(jnp.sum(column * column, axis=0, keepdims=True) + epsilon)
            unit = column * scale
            for k in range(i + 1, count):
                dot = jnp.sum(column * columns[k], axis=0, keepdims=True) * scale
                columns[k] = columns[k] - unit * dot
            dots = jnp.sum(column * work, axis=0, keepdims=True) * scale
            work = work - unit * dots
            done = jnp.where(lane == start + i, unit, done)
    basis[...] = done[:, :rank]
    basis_t[...] = done.T[:rank]


def right_kernel(basis_t, *refs):
    terms, outs = refs[:-PARTS], refs[-PARTS:]
    total = terms[0][...]
    for term in terms[1:]:
        total = total + term[...]
    both = jnp.dot(basis_t[...], total, precision=lax.Precision.HIGHEST, preferred_element_type=F32)
    size = outs[0].shape[0]
    for i, out in enumerate(outs):
        out[...] = both[i * size : (i + 1) * size]


def final_kernel(workers, merged, basis, *refs):
    *blocks, feedback, new_basis_t = refs
    count = len(blocks) // PARTS
    chunks = count // 2
    width = blocks[0].shape[1]
    mine = lax.axis_index("local")
    half = own_half()
    high, low = split(basis[...] * (1.0 / workers))
    left = jnp.concatenate([high, low, high], axis=1)
    for i in range(count):
        side = half if i < chunks else 1 - half
        start = (side * chunks + partner(mine, i % chunks, chunks)) * width
        span = pl.ds(pl.multiple_of(start, 128), width)
        piece = jnp.concatenate([block[...] for block in blocks[i::count]], axis=0)
        new_basis_t[:, span] = piece
        upper, lower = split(piece)
        right = jnp.concatenate([upper, upper, lower], axis=0)
        approx = jnp.dot(left, right, preferred_element_type=F32)
        feedback[:, span] = (merged[:, span] - approx).astype(BF16)


def body(gradient, feedback, basis_in):
    g, f = gradient[0], feedback[0]
    rows, columns = g.shape
    b = basis_in.T
    rank = b.shape[0]
    local, dp = lax.axis_size("local"), lax.axis_size("dp")
    groups = dp // 2
    half = columns // 2
    width = half // local

    def permute(value, along_local, step):
        pairs = []
        for x in range(local):
            for z in range(groups):
                to = (partner(x, step, local), z) if along_local else (x, partner(z, step, groups))
                flip = odd_bits(step, local if along_local else groups)
                for core in range(2):
                    pairs.append((x * dp + 2 * z + core, to[0] * dp + 2 * to[1] + (core ^ flip)))
        if partner(0, step, local if along_local else groups) != step:
            pairs = [(to, source) for source, to in pairs]
        return lax.ppermute(value, AXES, pairs)

    def swap(value):
        return lax.ppermute(value, AXES, [(i, i ^ 1) for i in range(local * dp)])

    def total_over(value, along_local, direct=False):
        size = local if along_local else groups
        double = not direct and not size & (size - 1)
        first = value
        step = 1
        while step < size:
            other = permute(value if double else first, along_local, step)
            value = value + other
            step = 2 * step if double else step + 1
        return value

    pieces = PIECES if columns % (128 * PIECES) == 0 else 2
    g, f, b = (pltpu.with_memory_space_constraint(x, pltpu.HBM) for x in (g, f, b))
    left, merged, send = call(
        left_kernel, [((rank, rows), F32), ((rows, columns), F32), ((rows, half), F32)],
        g, f, b, flops=1 << 27, limit=16,
        scratch=[VMEM(g.shape, g.dtype), VMEM(f.shape, f.dtype), VMEM(b.shape, b.dtype),
                 pltpu.SemaphoreType.DMA((3, pieces))],
        space=pltpu.HBM,
    )
    got = swap(send)
    left = total_over(left, True, direct=True)
    chunks = call(pair_kernel, [((rows, width), F32)] * local, merged, got)
    terms = [chunks[0]] + [permute(chunks[s], True, s) for s in range(1, local)]
    left = total_over(left, False)
    basis, basis_t = call(
        functools.partial(gram_schmidt_kernel, 4),
        [((rows, rank), F32), ((rank, rows), F32)],
        left, swap(left), flops=1 << 26,
    )
    rights = call(right_kernel, [((rank // PARTS, width), F32)] * PARTS, basis_t, *terms, flops=1 << 25)
    blocks = []
    for right in rights:
        own = total_over(right, False)
        gathered = [own] + [permute(own, True, s) for s in range(1, local)]
        blocks += gathered + [swap(block) for block in gathered]
    new_feedback, new_basis_t = call(
        functools.partial(final_kernel, local * dp),
        [((rows, columns), BF16), ((rank, columns), F32)],
        merged, basis, *blocks, flops=1 << 27, limit=16,
    )
    return (new_feedback[None], new_basis_t.T)


def solution(mesh):
    return jax.shard_map(
        body,
        mesh=mesh,
        in_specs=(P(("local", "dp"), None, None), P(("local", "dp"), None, None), P()),
        out_specs=(P(("local", "dp"), None, None), P()),
        check_vma=False,
    )
```

```python
import functools

import jax
import jax.numpy as jnp
from jax import lax
from jax.experimental import pallas as pl
from jax.experimental.pallas import tpu as pltpu
from jax.sharding import PartitionSpec as P


epsilon = 1e-06
AXES = ("local", "dp")
F32, BF16 = jnp.float32, jnp.bfloat16
VMEM = pltpu.VMEM
PARTS = 2


def call(kernel, outs, *args, flops=1 << 20, limit=12, scratch=(), space=VMEM, target=VMEM, aliased=0):
    many = isinstance(outs, list)
    shapes = [jax.ShapeDtypeStruct(s, d) for s, d in (outs if many else [outs])]
    size = sum(a.size * a.dtype.itemsize for a in args)
    plain = len(args) - aliased
    result = pl.pallas_call(
        kernel,
        out_shape=shapes,
        in_specs=[pl.BlockSpec(memory_space=space)] * plain + [pl.BlockSpec(memory_space=target)] * aliased,
        out_specs=[pl.BlockSpec(memory_space=target)] * len(shapes),
        input_output_aliases={plain + i: i for i in range(aliased)},
        scratch_shapes=scratch,
        compiler_params=pltpu.CompilerParams(vmem_limit_bytes=limit << 20),
        cost_estimate=pl.CostEstimate(flops=flops, bytes_accessed=size, transcendentals=0),
    )(*args)
    return result if many else result[0]


def split(value):
    high = value.astype(BF16)
    return high, (value - high.astype(F32)).astype(BF16)


def partner(index, step, size):
    if size & (size - 1):
        return (index + step) % size
    return index ^ step


def odd_bits(index, size):
    total = 0
    while size > 1 and not size & (size - 1):
        total, index, size = total + index % 2, index // 2, size // 2
    return total % 2


def own_half():
    local, dp = lax.axis_size("local"), lax.axis_size("dp")
    place = lax.axis_index("dp")
    return (place % 2 + odd_bits(lax.axis_index("local"), local) + odd_bits(place // 2, dp // 2)) % 2


def load_kernel(g, f, gv, fv, send, sems):
    copies = [pltpu.make_async_copy(x, y, sems.at[i]) for i, (x, y) in enumerate(((g, gv), (f, fv)))]
    for copy in copies:
        copy.start()
    for copy in copies:
        copy.wait()
    width = send.shape[1]
    half = own_half()
    for side in range(2):

        @pl.when(half == 1 - side)
        def _():
            span = slice(side * width, (side + 1) * width)
            send[...] = gv[:, span].astype(F32) + fv[:, span].astype(F32)


def left_kernel(g, f, b, left):
    rank = b.shape[0]
    high, low = split(b[...])
    basis = jnp.concatenate([high, low], axis=0)
    dims = (((1,), (1,)), ((), ()))
    both = lax.dot_general(basis, g[...], dims, preferred_element_type=F32)
    both += lax.dot_general(basis, f[...], dims, preferred_element_type=F32)
    left[...] = both[:rank] + both[rank:]


def pair_kernel(g, f, got, *outs):
    width = outs[0].shape[1]
    mine = lax.axis_index("local")
    start = own_half() * got.shape[1]
    for step, out in enumerate(outs):
        inner = pl.multiple_of(partner(mine, step, len(outs)) * width, 128)
        span = pl.ds(pl.multiple_of(start + inner, 128), width)
        out[...] = g[:, span].astype(F32) + f[:, span].astype(F32) + got[:, pl.ds(inner, width)]


def gram_schmidt_kernel(block, a, b, basis, basis_t):
    rank, rows = a.shape
    lanes = 128
    total = jnp.concatenate([a[...] + b[...], jnp.zeros((lanes - rank, rows), F32)], axis=0)
    work = total.T
    lane = lax.broadcasted_iota(jnp.int32, (rows, lanes), 1)
    done = jnp.zeros((rows, lanes), F32)
    for start in range(0, rank, block):
        count = min(block, rank - start)
        columns = [jnp.broadcast_to(work[:, start + i : start + i + 1], (rows, lanes)) for i in range(count)]
        for i in range(count):
            column = columns[i]
            scale = lax.rsqrt(jnp.sum(column * column, axis=0, keepdims=True) + epsilon)
            unit = column * scale
            for k in range(i + 1, count):
                dot = jnp.sum(column * columns[k], axis=0, keepdims=True) * scale
                columns[k] = columns[k] - unit * dot
            dots = jnp.sum(column * work, axis=0, keepdims=True) * scale
            work = work - unit * dots
            done = jnp.where(lane == start + i, unit, done)
    basis[...] = done[:, :rank]
    basis_t[...] = done.T[:rank]


def right_kernel(basis_t, *refs):
    terms, outs = refs[:-PARTS], refs[-PARTS:]
    total = terms[0][...]
    for term in terms[1:]:
        total = total + term[...]
    both = jnp.dot(basis_t[...], total, precision=lax.Precision.HIGHEST, preferred_element_type=F32)
    size = outs[0].shape[0]
    for i, out in enumerate(outs):
        out[...] = both[i * size : (i + 1) * size]


def final_kernel(workers, other, g, f, basis, *refs):
    feedback, new_basis_t, staged, sems = refs[-4:]
    blocks = refs[: len(refs) - (6 if other else 4)]
    chunks = len(blocks) // PARTS
    size, width = blocks[0].shape
    mine = lax.axis_index("local")
    side = (own_half() + other) % 2
    high, low = split(basis[...] * (1.0 / workers))
    left = jnp.concatenate([high, low, high], axis=1)
    copies = []

    def put(source, target, i, j):
        copies.append(pltpu.make_async_copy(source, target, sems.at[i, j]))
        copies[-1].start()

    spans = []
    for i in range(chunks):
        start = (side * chunks + partner(mine, i, chunks)) * width
        spans.append(pl.ds(pl.multiple_of(start, 128), width))
        for part in range(PARTS):
            rows = pl.ds(part * size, size)
            put(blocks[part * chunks + i], new_basis_t.at[rows, spans[i]], i, part)
    for i, span in enumerate(spans):
        upper, lower = split(jnp.concatenate([block[...] for block in blocks[i::chunks]], axis=0))
        right = jnp.concatenate([upper, upper, lower], axis=0)
        approx = jnp.dot(left, right, preferred_element_type=F32)
        merged = g[:, span].astype(F32) + f[:, span].astype(F32)
        staged[:, i * width : (i + 1) * width] = (merged - approx).astype(BF16)
        put(staged.at[:, i * width : (i + 1) * width], feedback.at[:, span], i, PARTS)
    for copy in copies:
        copy.wait()


def body(gradient, feedback, basis_in):
    g, f = gradient[0], feedback[0]
    rows, columns = g.shape
    b = basis_in.T
    rank = b.shape[0]
    local, dp = lax.axis_size("local"), lax.axis_size("dp")
    groups = dp // 2
    half = columns // 2
    width = half // local

    def permute(value, along_local, step):
        pairs = []
        for x in range(local):
            for z in range(groups):
                to = (partner(x, step, local), z) if along_local else (x, partner(z, step, groups))
                flip = odd_bits(step, local if along_local else groups)
                for core in range(2):
                    pairs.append((x * dp + 2 * z + core, to[0] * dp + 2 * to[1] + (core ^ flip)))
        if partner(0, step, local if along_local else groups) != step:
            pairs = [(to, source) for source, to in pairs]
        return lax.ppermute(value, AXES, pairs)

    def swap(value):
        return lax.ppermute(value, AXES, [(i, i ^ 1) for i in range(local * dp)])

    def total_over(value, along_local, direct=False):
        size = local if along_local else groups
        double = not direct and not size & (size - 1)
        first = value
        step = 1
        while step < size:
            other = permute(value if double else first, along_local, step)
            value = value + other
            step = 2 * step if double else step + 1
        return value

    g, f, send = call(
        load_kernel,
        [(g.shape, g.dtype), (f.shape, f.dtype), ((rows, half), F32)],
        *(pltpu.with_memory_space_constraint(x, pltpu.HBM) for x in (g, f)),
        scratch=[pltpu.SemaphoreType.DMA((2,))], space=pltpu.HBM,
    )
    left = call(left_kernel, ((rank, rows), F32), g, f, b, flops=1 << 27)
    got = swap(send)
    left = total_over(left, True, direct=True)
    chunks = call(pair_kernel, [((rows, width), F32)] * local, g, f, got)
    terms = [chunks[0]] + [permute(chunks[s], True, s) for s in range(1, local)]
    left = total_over(left, False)
    basis, basis_t = call(
        functools.partial(gram_schmidt_kernel, 4),
        [((rows, rank), F32), ((rank, rows), F32)],
        left, swap(left), flops=1 << 26,
    )
    rights = call(right_kernel, [((rank // PARTS, width), F32)] * PARTS, basis_t, *terms, flops=1 << 25)
    blocks, others = [], []
    for right in rights:
        own = total_over(right, False)
        gathered = [own] + [permute(own, True, s) for s in range(1, local)]
        blocks += gathered
        others += [swap(block) for block in gathered]
    outs = ()
    for other, arrays in enumerate((blocks, others)):
        outs = call(
            functools.partial(final_kernel, local * dp, other),
            [((rows, columns), BF16), ((rank, columns), F32)],
            g, f, basis, *arrays, *outs, flops=1 << 27, aliased=len(outs), target=pltpu.HBM,
            scratch=[VMEM((rows, half), BF16), pltpu.SemaphoreType.DMA((local, PARTS + 1))],
        )
    return (outs[0][None], outs[1].T)


def solution(mesh):
    return jax.shard_map(
        body,
        mesh=mesh,
        in_specs=(P(("local", "dp"), None, None), P(("local", "dp"), None, None), P()),
        out_specs=(P(("local", "dp"), None, None), P()),
        check_vma=False,
    )
```

```python
import functools

import jax
import jax.numpy as jnp
from jax import lax
from jax.experimental import pallas as pl
from jax.experimental.pallas import tpu as pltpu
from jax.sharding import PartitionSpec as P


epsilon = 1e-06
AXES = ("local", "dp")
F32, BF16 = jnp.float32, jnp.bfloat16
VMEM = pltpu.VMEM
PARTS = 2


def call(kernel, outs, *args, flops=1 << 20, limit=12, scratch=(), space=VMEM, target=VMEM, aliased=0):
    many = isinstance(outs, list)
    shapes = [jax.ShapeDtypeStruct(s, d) for s, d in (outs if many else [outs])]
    size = sum(a.size * a.dtype.itemsize for a in args)
    plain = len(args) - aliased
    result = pl.pallas_call(
        kernel,
        out_shape=shapes,
        in_specs=[pl.BlockSpec(memory_space=space)] * plain + [pl.BlockSpec(memory_space=target)] * aliased,
        out_specs=[pl.BlockSpec(memory_space=target)] * len(shapes),
        input_output_aliases={plain + i: i for i in range(aliased)},
        scratch_shapes=scratch,
        compiler_params=pltpu.CompilerParams(vmem_limit_bytes=limit << 20),
        cost_estimate=pl.CostEstimate(flops=flops, bytes_accessed=size, transcendentals=0),
    )(*args)
    return result if many else result[0]


def split(value):
    high = value.astype(BF16)
    return high, (value - high.astype(F32)).astype(BF16)


def partner(index, step, size):
    if size & (size - 1):
        return (index + step) % size
    return index ^ step


def odd_bits(index, size):
    total = 0
    while size > 1 and not size & (size - 1):
        total, index, size = total + index % 2, index // 2, size // 2
    return total % 2


def own_half():
    local, dp = lax.axis_size("local"), lax.axis_size("dp")
    place = lax.axis_index("dp")
    return (place % 2 + odd_bits(lax.axis_index("local"), local) + odd_bits(place // 2, dp // 2)) % 2


def load_kernel(g, f, gv, fv, send, sems):
    copies = [pltpu.make_async_copy(x, y, sems.at[i]) for i, (x, y) in enumerate(((g, gv), (f, fv)))]
    for copy in copies:
        copy.start()
    for copy in copies:
        copy.wait()
    width = send.shape[1]
    half = own_half()
    for side in range(2):

        @pl.when(half == 1 - side)
        def _():
            span = slice(side * width, (side + 1) * width)
            send[...] = gv[:, span].astype(F32) + fv[:, span].astype(F32)


def left_kernel(g, f, b, left):
    rank = b.shape[0]
    high, low = split(b[...])
    basis = jnp.concatenate([high, low], axis=0)
    dims = (((1,), (1,)), ((), ()))
    both = lax.dot_general(basis, g[...], dims, preferred_element_type=F32)
    both += lax.dot_general(basis, f[...], dims, preferred_element_type=F32)
    left[...] = both[:rank] + both[rank:]


def pair_kernel(g, f, got, *outs):
    width = outs[0].shape[1]
    mine = lax.axis_index("local")
    start = own_half() * got.shape[1]
    for step, out in enumerate(outs):
        inner = pl.multiple_of(partner(mine, step, len(outs)) * width, 128)
        span = pl.ds(pl.multiple_of(start + inner, 128), width)
        out[...] = g[:, span].astype(F32) + f[:, span].astype(F32) + got[:, pl.ds(inner, width)]


def gram_schmidt_kernel(block, a, b, basis, basis_t):
    rank, rows = a.shape
    lanes = 128
    total = jnp.concatenate([a[...] + b[...], jnp.zeros((lanes - rank, rows), F32)], axis=0)
    work = total.T
    lane = lax.broadcasted_iota(jnp.int32, (rows, lanes), 1)
    done = jnp.zeros((rows, lanes), F32)
    for start in range(0, rank, block):
        count = min(block, rank - start)
        columns = [jnp.broadcast_to(work[:, start + i : start + i + 1], (rows, lanes)) for i in range(count)]
        for i in range(count):
            column = columns[i]
            scale = lax.rsqrt(jnp.sum(column * column, axis=0, keepdims=True) + epsilon)
            unit = column * scale
            for k in range(i + 1, count):
                dot = jnp.sum(column * columns[k], axis=0, keepdims=True) * scale
                columns[k] = columns[k] - unit * dot
            dots = jnp.sum(column * work, axis=0, keepdims=True) * scale
            work = work - unit * dots
            done = jnp.where(lane == start + i, unit, done)
    basis[...] = done[:, :rank]
    basis_t[...] = done.T[:rank]


def right_kernel(basis_t, *refs):
    terms, outs = refs[:-PARTS], refs[-PARTS:]
    total = terms[0][...]
    for term in terms[1:]:
        total = total + term[...]
    both = jnp.dot(basis_t[...], total, precision=lax.Precision.HIGHEST, preferred_element_type=F32)
    size = outs[0].shape[0]
    for i, out in enumerate(outs):
        out[...] = both[i * size : (i + 1) * size]


def pack_kernel(*refs):
    *blocks, out = refs
    size = blocks[0].shape[0]
    for i, block in enumerate(blocks):
        out[i * size : (i + 1) * size] = block[...]


def final_kernel(workers, other, g, f, basis, *refs):
    parts = refs[:PARTS]
    feedback, new_basis_t, staged, sems = refs[-4:]
    chunks = sems.shape[0]
    size, width = parts[0].shape[0] // chunks, parts[0].shape[1]
    mine = lax.axis_index("local")
    side = (own_half() + other) % 2
    high, low = split(basis[...] * (1.0 / workers))
    left = jnp.concatenate([high, low, high], axis=1)
    copies = []

    def put(source, target, i, j):
        copies.append(pltpu.make_async_copy(source, target, sems.at[i, j]))
        copies[-1].start()

    spans = []
    for i in range(chunks):
        start = (side * chunks + partner(mine, i, chunks)) * width
        spans.append(pl.ds(pl.multiple_of(start, 128), width))
        for j, part in enumerate(parts):
            put(part.at[pl.ds(i * size, size)], new_basis_t.at[pl.ds(j * size, size), spans[i]], i, j)
    for i, span in enumerate(spans):
        piece = jnp.concatenate([part[i * size : (i + 1) * size] for part in parts], axis=0)
        upper, lower = split(piece)
        right = jnp.concatenate([upper, upper, lower], axis=0)
        approx = jnp.dot(left, right, preferred_element_type=F32)
        merged = g[:, span].astype(F32) + f[:, span].astype(F32)
        staged[:, i * width : (i + 1) * width] = (merged - approx).astype(BF16)
        put(staged.at[:, i * width : (i + 1) * width], feedback.at[:, span], i, PARTS)
    for copy in copies:
        copy.wait()


def body(gradient, feedback, basis_in):
    g, f = gradient[0], feedback[0]
    rows, columns = g.shape
    b = basis_in.T
    rank = b.shape[0]
    local, dp = lax.axis_size("local"), lax.axis_size("dp")
    groups = dp // 2
    half = columns // 2
    width = half // local

    def permute(value, along_local, step):
        pairs = []
        for x in range(local):
            for z in range(groups):
                to = (partner(x, step, local), z) if along_local else (x, partner(z, step, groups))
                flip = odd_bits(step, local if along_local else groups)
                for core in range(2):
                    pairs.append((x * dp + 2 * z + core, to[0] * dp + 2 * to[1] + (core ^ flip)))
        if partner(0, step, local if along_local else groups) != step:
            pairs = [(to, source) for source, to in pairs]
        return lax.ppermute(value, AXES, pairs)

    def swap(value):
        return lax.ppermute(value, AXES, [(i, i ^ 1) for i in range(local * dp)])

    def total_over(value, along_local, direct=False):
        size = local if along_local else groups
        double = not direct and not size & (size - 1)
        first = value
        step = 1
        while step < size:
            other = permute(value if double else first, along_local, step)
            value = value + other
            step = 2 * step if double else step + 1
        return value

    def gather(own, turn):
        if local & (local - 1):
            return [own] + [permute(own, True, s) for s in range(1, local)]
        blocks = {0: own}
        steps = [1 << i for i in range(local.bit_length() - 1)]
        for step in steps[::-1] if turn else steps:
            new = {}
            for place, block in blocks.items():
                new[place ^ step] = permute(block, True, step)
            blocks.update(new)
        return [blocks[place] for place in range(local)]

    g, f, send = call(
        load_kernel,
        [(g.shape, g.dtype), (f.shape, f.dtype), ((rows, half), F32)],
        *(pltpu.with_memory_space_constraint(x, pltpu.HBM) for x in (g, f)),
        scratch=[pltpu.SemaphoreType.DMA((2,))], space=pltpu.HBM,
    )
    left = call(left_kernel, ((rank, rows), F32), g, f, b, flops=1 << 27)
    got = swap(send)
    left = total_over(left, True, direct=True)
    chunks = call(pair_kernel, [((rows, width), F32)] * local, g, f, got)
    terms = [chunks[0]] + [permute(chunks[s], True, s) for s in range(1, local)]
    left = total_over(left, False)
    basis, basis_t = call(
        functools.partial(gram_schmidt_kernel, 4),
        [((rows, rank), F32), ((rank, rows), F32)],
        left, swap(left), flops=1 << 26,
    )
    rights = call(right_kernel, [((rank // PARTS, width), F32)] * PARTS, basis_t, *terms, flops=1 << 25)
    blocks, others = [], []
    for part, right in enumerate(rights):
        own = total_over(right, False)
        gathered = gather(own, part % 2)
        blocks.append(call(pack_kernel, ((local * own.shape[0], width), F32), *gathered))
        others.append(swap(blocks[-1]))
    outs = ()
    for other, arrays in enumerate((blocks, others)):
        outs = call(
            functools.partial(final_kernel, local * dp, other),
            [((rows, columns), BF16), ((rank, columns), F32)],
            g, f, basis, *arrays, *outs, flops=1 << 27, aliased=len(outs), target=pltpu.HBM,
            scratch=[VMEM((rows, half), BF16), pltpu.SemaphoreType.DMA((local, PARTS + 1))],
        )
    return (outs[0][None], outs[1].T)


def solution(mesh):
    return jax.shard_map(
        body,
        mesh=mesh,
        in_specs=(P(("local", "dp"), None, None), P(("local", "dp"), None, None), P()),
        out_specs=(P(("local", "dp"), None, None), P()),
        check_vma=False,
    )
```

```python
import functools

import jax
import jax.numpy as jnp
from jax import lax
from jax.experimental import pallas as pl
from jax.experimental.pallas import tpu as pltpu
from jax.sharding import PartitionSpec as P


epsilon = 1e-06
AXES = ("local", "dp")
F32, BF16 = jnp.float32, jnp.bfloat16
VMEM = pltpu.VMEM
PARTS = 2


def call(kernel, outs, *args, flops=1 << 20, limit=12, scratch=(), space=VMEM, target=VMEM, aliased=0):
    many = isinstance(outs, list)
    shapes = [jax.ShapeDtypeStruct(s, d) for s, d in (outs if many else [outs])]
    size = sum(a.size * a.dtype.itemsize for a in args)
    plain = len(args) - aliased
    result = pl.pallas_call(
        kernel,
        out_shape=shapes,
        in_specs=[pl.BlockSpec(memory_space=space)] * plain + [pl.BlockSpec(memory_space=target)] * aliased,
        out_specs=[pl.BlockSpec(memory_space=target)] * len(shapes),
        input_output_aliases={plain + i: i for i in range(aliased)},
        scratch_shapes=scratch,
        compiler_params=pltpu.CompilerParams(vmem_limit_bytes=limit << 20),
        cost_estimate=pl.CostEstimate(flops=flops, bytes_accessed=size, transcendentals=0),
    )(*args)
    return result if many else result[0]


def split(value):
    high = value.astype(BF16)
    return high, (value - high.astype(F32)).astype(BF16)


def partner(index, step, size):
    if size & (size - 1):
        return (index + step) % size
    return index ^ step


def odd_bits(index, size):
    total = 0
    while size > 1 and not size & (size - 1):
        total, index, size = total + index % 2, index // 2, size // 2
    return total % 2


def own_half():
    local, dp = lax.axis_size("local"), lax.axis_size("dp")
    place = lax.axis_index("dp")
    return (place % 2 + odd_bits(lax.axis_index("local"), local) + odd_bits(place // 2, dp // 2)) % 2


def load_kernel(g, f, gv, fv, send, sems):
    copies = [pltpu.make_async_copy(x, y, sems.at[i]) for i, (x, y) in enumerate(((g, gv), (f, fv)))]
    for copy in copies:
        copy.start()
    for copy in copies:
        copy.wait()
    width = send.shape[1]
    half = own_half()
    for side in range(2):

        @pl.when(half == 1 - side)
        def _():
            span = slice(side * width, (side + 1) * width)
            send[...] = gv[:, span].astype(F32) + fv[:, span].astype(F32)


def left_kernel(g, f, b, left):
    rank = b.shape[0]
    high, low = split(b[...])
    basis = jnp.concatenate([high, low], axis=0)
    dims = (((1,), (1,)), ((), ()))
    both = lax.dot_general(basis, g[...], dims, preferred_element_type=F32)
    both += lax.dot_general(basis, f[...], dims, preferred_element_type=F32)
    left[...] = both[:rank] + both[rank:]


def pair_kernel(g, f, got, *outs):
    width = outs[0].shape[1]
    mine = lax.axis_index("local")
    start = own_half() * got.shape[1]
    for step, out in enumerate(outs):
        inner = pl.multiple_of(partner(mine, step, len(outs)) * width, 128)
        span = pl.ds(pl.multiple_of(start + inner, 128), width)
        out[...] = g[:, span].astype(F32) + f[:, span].astype(F32) + got[:, pl.ds(inner, width)]


def column_sum(value):
    rows = value.shape[0]
    if rows % 8:
        return jnp.sum(value, axis=0, keepdims=True)
    terms = [value[i : i + 8] for i in range(0, rows, 8)]
    while len(terms) > 1:
        terms = [sum(terms[i + 1 : i + 2], terms[i]) for i in range(0, len(terms), 2)]
    return jnp.sum(terms[0], axis=0, keepdims=True)


def gram_schmidt_kernel(window, a, b, basis, basis_t):
    rank, rows = a.shape
    lanes = 128
    total = jnp.concatenate([a[...] + b[...], jnp.zeros((lanes - rank, rows), F32)], axis=0)
    work = total.T
    lane = lax.broadcasted_iota(jnp.int32, (1, lanes), 1)

    def spread(index):
        return jnp.broadcast_to(work[:, index : index + 1], (rows, lanes))

    columns = {index: spread(index) for index in range(min(window, rank))}
    for index in range(rank):
        column = columns.pop(index)
        scale = lax.rsqrt(column_sum(column * column) + epsilon)
        unit = column * scale
        for later in columns:
            columns[later] = columns[later] - unit * (column_sum(column * columns[later]) * scale)
        dots = jnp.where(lane > index, column_sum(column * work) * scale, 0.0)
        work = jnp.where(lane == index, unit, work - unit * dots)
        if index + window < rank:
            columns[index + window] = spread(index + window)
    basis[...] = work[:, :rank]
    basis_t[...] = work.T[:rank]


def right_kernel(basis_t, *refs):
    terms, outs = refs[:-PARTS], refs[-PARTS:]
    total = terms[0][...]
    for term in terms[1:]:
        total = total + term[...]
    both = jnp.dot(basis_t[...], total, precision=lax.Precision.HIGHEST, preferred_element_type=F32)
    size = outs[0].shape[0]
    for i, out in enumerate(outs):
        out[...] = both[i * size : (i + 1) * size]


def pack_kernel(*refs):
    *blocks, out = refs
    size = blocks[0].shape[0]
    for i, block in enumerate(blocks):
        out[i * size : (i + 1) * size] = block[...]


def final_kernel(workers, other, g, f, basis, *refs):
    parts = refs[:PARTS]
    feedback, new_basis_t, staged, sems = refs[-4:]
    chunks = sems.shape[0]
    size, width = parts[0].shape[0] // chunks, parts[0].shape[1]
    mine = lax.axis_index("local")
    side = (own_half() + other) % 2
    high, low = split(basis[...] * (1.0 / workers))
    left = jnp.concatenate([high, low, high], axis=1)
    copies = []

    def put(source, target, i, j):
        copies.append(pltpu.make_async_copy(source, target, sems.at[i, j]))
        copies[-1].start()

    spans = []
    for i in range(chunks):
        start = (side * chunks + partner(mine, i, chunks)) * width
        spans.append(pl.ds(pl.multiple_of(start, 128), width))
        for j, part in enumerate(parts):
            put(part.at[pl.ds(i * size, size)], new_basis_t.at[pl.ds(j * size, size), spans[i]], i, j)
    for i, span in enumerate(spans):
        piece = jnp.concatenate([part[i * size : (i + 1) * size] for part in parts], axis=0)
        upper, lower = split(piece)
        right = jnp.concatenate([upper, upper, lower], axis=0)
        approx = jnp.dot(left, right, preferred_element_type=F32)
        merged = g[:, span].astype(F32) + f[:, span].astype(F32)
        staged[:, i * width : (i + 1) * width] = (merged - approx).astype(BF16)
        put(staged.at[:, i * width : (i + 1) * width], feedback.at[:, span], i, PARTS)
    for copy in copies:
        copy.wait()


def body(gradient, feedback, basis_in):
    g, f = gradient[0], feedback[0]
    rows, columns = g.shape
    b = basis_in.T
    rank = b.shape[0]
    local, dp = lax.axis_size("local"), lax.axis_size("dp")
    groups = dp // 2
    half = columns // 2
    width = half // local

    def permute(value, along_local, step, cross=None):
        pairs = []
        for x in range(local):
            for z in range(groups):
                to = (partner(x, step, local), z) if along_local else (x, partner(z, step, groups))
                flip = odd_bits(step, local if along_local else groups) if cross is None else cross
                for core in range(2):
                    pairs.append((x * dp + 2 * z + core, to[0] * dp + 2 * to[1] + (core ^ flip)))
        if partner(0, step, local if along_local else groups) != step:
            pairs = [(to, source) for source, to in pairs]
        return lax.ppermute(value, AXES, pairs)

    def swap(value):
        return lax.ppermute(value, AXES, [(i, i ^ 1) for i in range(local * dp)])

    def total_over(value, along_local, direct=False, cross=None, turn=0):
        size = local if along_local else groups
        double = not direct and not size & (size - 1)
        first = value
        steps = [1 << i for i in range(size.bit_length() - 1)] if double else range(1, size)
        for step in steps[::-1] if turn else steps:
            other = permute(value if double else first, along_local, step, cross)
            value = value + other
        return value

    def gather(own, turn):
        if local & (local - 1):
            return [own] + [permute(own, True, s) for s in range(1, local)]
        blocks = {0: own}
        steps = [1 << i for i in range(local.bit_length() - 1)]
        for step in steps[::-1] if turn else steps:
            new = {}
            for place, block in blocks.items():
                new[place ^ step] = permute(block, True, step)
            blocks.update(new)
        return [blocks[place] for place in range(local)]

    g, f, send = call(
        load_kernel,
        [(g.shape, g.dtype), (f.shape, f.dtype), ((rows, half), F32)],
        *(pltpu.with_memory_space_constraint(x, pltpu.HBM) for x in (g, f)),
        scratch=[pltpu.SemaphoreType.DMA((2,))], space=pltpu.HBM,
    )
    left = call(left_kernel, ((rank, rows), F32), g, f, b, flops=1 << 27)
    got = swap(send)
    left = total_over(left, True, direct=True, cross=1)
    chunks = call(pair_kernel, [((rows, width), F32)] * local, g, f, got)
    terms = [chunks[0]] + [permute(chunks[s], True, s) for s in range(1, local)]
    left = total_over(left, False, cross=1)
    basis, basis_t = call(
        functools.partial(gram_schmidt_kernel, 4),
        [((rows, rank), F32), ((rank, rows), F32)],
        left, swap(left), flops=1 << 26,
    )
    rights = call(right_kernel, [((rank // PARTS, width), F32)] * PARTS, basis_t, *terms, flops=1 << 25)
    blocks, others = [], []
    for part, right in enumerate(rights):
        own = total_over(right, False, turn=part % 2)
        gathered = gather(own, part % 2)
        blocks.append(call(pack_kernel, ((local * own.shape[0], width), F32), *gathered))
        others.append(swap(blocks[-1]))
    outs = ()
    for other, arrays in enumerate((blocks, others)):
        outs = call(
            functools.partial(final_kernel, local * dp, other),
            [((rows, columns), BF16), ((rank, columns), F32)],
            g, f, basis, *arrays, *outs, flops=1 << 27, aliased=len(outs), target=pltpu.HBM,
            scratch=[VMEM((rows, half), BF16), pltpu.SemaphoreType.DMA((local, PARTS + 1))],
        )
    return (outs[0][None], outs[1].T)


def solution(mesh):
    return jax.shard_map(
        body,
        mesh=mesh,
        in_specs=(P(("local", "dp"), None, None), P(("local", "dp"), None, None), P()),
        out_specs=(P(("local", "dp"), None, None), P()),
        check_vma=False,
    )
```

```python
import functools

import jax
import jax.numpy as jnp
from jax import lax
from jax.experimental import pallas as pl
from jax.experimental.pallas import tpu as pltpu
from jax.sharding import PartitionSpec as P


epsilon = 1e-06
AXES = ("local", "dp")
F32, BF16 = jnp.float32, jnp.bfloat16
VMEM = pltpu.VMEM
PARTS = 2


def call(kernel, outs, *args, flops=1 << 20, limit=12, scratch=(), space=VMEM, target=VMEM, aliased=0):
    many = isinstance(outs, list)
    shapes = [jax.ShapeDtypeStruct(s, d) for s, d in (outs if many else [outs])]
    size = sum(a.size * a.dtype.itemsize for a in args)
    plain = len(args) - aliased
    result = pl.pallas_call(
        kernel,
        out_shape=shapes,
        in_specs=[pl.BlockSpec(memory_space=space)] * plain + [pl.BlockSpec(memory_space=target)] * aliased,
        out_specs=[pl.BlockSpec(memory_space=target)] * len(shapes),
        input_output_aliases={plain + i: i for i in range(aliased)},
        scratch_shapes=scratch,
        compiler_params=pltpu.CompilerParams(vmem_limit_bytes=limit << 20),
        cost_estimate=pl.CostEstimate(flops=flops, bytes_accessed=size, transcendentals=0),
    )(*args)
    return result if many else result[0]


def split(value):
    high = value.astype(BF16)
    return high, (value - high.astype(F32)).astype(BF16)


def partner(index, step, size):
    if size & (size - 1):
        return (index + step) % size
    return index ^ step


def odd_bits(index, size):
    total = 0
    while size > 1 and not size & (size - 1):
        total, index, size = total + index % 2, index // 2, size // 2
    return total % 2


def own_half():
    local, dp = lax.axis_size("local"), lax.axis_size("dp")
    place = lax.axis_index("dp")
    return (place % 2 + odd_bits(lax.axis_index("local"), local) + odd_bits(place // 2, dp // 2)) % 2


def load_kernel(g, f, gv, fv, send, sems):
    copies = [pltpu.make_async_copy(x, y, sems.at[i]) for i, (x, y) in enumerate(((g, gv), (f, fv)))]
    for copy in copies:
        copy.start()
    for copy in copies:
        copy.wait()
    width = send.shape[1]
    half = own_half()
    for side in range(2):

        @pl.when(half == 1 - side)
        def _():
            span = slice(side * width, (side + 1) * width)
            send[...] = gv[:, span].astype(F32) + fv[:, span].astype(F32)


def left_kernel(g, f, b, left):
    rank = b.shape[0]
    high, low = split(b[...])
    basis = jnp.concatenate([high, low], axis=0)
    dims = (((1,), (1,)), ((), ()))
    both = lax.dot_general(basis, g[...], dims, preferred_element_type=F32)
    both += lax.dot_general(basis, f[...], dims, preferred_element_type=F32)
    left[...] = both[:rank] + both[rank:]


def pair_kernel(g, f, got, *outs):
    width = outs[0].shape[1]
    mine = lax.axis_index("local")
    start = own_half() * got.shape[1]
    for step, out in enumerate(outs):
        inner = pl.multiple_of(partner(mine, step, len(outs)) * width, 128)
        span = pl.ds(pl.multiple_of(start + inner, 128), width)
        out[...] = g[:, span].astype(F32) + f[:, span].astype(F32) + got[:, pl.ds(inner, width)]


def column_sum(value):
    rows = value.shape[0]
    if rows % 8:
        return jnp.sum(value, axis=0, keepdims=True)
    terms = [value[i : i + 8] for i in range(0, rows, 8)]
    while len(terms) > 1:
        terms = [sum(terms[i + 1 : i + 2], terms[i]) for i in range(0, len(terms), 2)]
    return jnp.sum(terms[0], axis=0, keepdims=True)


def gram_schmidt_kernel(window, a, b, basis, basis_t):
    rank, rows = a.shape
    lanes = 128
    total = jnp.concatenate([a[...] + b[...], jnp.zeros((lanes - rank, rows), F32)], axis=0)
    work = total.T
    lane = lax.broadcasted_iota(jnp.int32, (1, lanes), 1)

    def spread(index):
        return jnp.broadcast_to(work[:, index : index + 1], (rows, lanes))

    columns = {index: spread(index) for index in range(min(window, rank))}
    for index in range(rank):
        column = columns.pop(index)
        scale = lax.rsqrt(column_sum(column * column) + epsilon)
        unit = column * scale
        for later in columns:
            columns[later] = columns[later] - unit * (column_sum(column * columns[later]) * scale)
        dots = jnp.where(lane > index, column_sum(column * work) * scale, 0.0)
        work = jnp.where(lane == index, unit, work - unit * dots)
        if index + window < rank:
            columns[index + window] = spread(index + window)
    basis[...] = work[:, :rank]
    basis_t[...] = work.T[:rank]


def right_kernel(basis_t, *refs):
    terms, outs = refs[:-PARTS], refs[-PARTS:]
    total = terms[0][...]
    for term in terms[1:]:
        total = total + term[...]
    both = jnp.dot(basis_t[...], total, precision=lax.Precision.HIGHEST, preferred_element_type=F32)
    size = outs[0].shape[0]
    for i, out in enumerate(outs):
        out[...] = both[i * size : (i + 1) * size]


def pack_kernel(*refs):
    *blocks, out = refs
    size = blocks[0].shape[0]
    for i, block in enumerate(blocks):
        out[i * size : (i + 1) * size] = block[...]


def final_kernel(workers, plan, g, f, basis, *refs):
    feedback, new_basis_t, staged, sems = refs[-4:]
    rank = basis.shape[1]
    width = refs[0].shape[1]
    local = lax.axis_size("local")
    mine = lax.axis_index("local")
    high, low = split(basis[...] * (1.0 / workers))
    left = jnp.concatenate([high, low, high], axis=1)
    work, copies = [], []

    def put(source, target, i, j):
        copies.append(pltpu.make_async_copy(source, target, sems.at[i, j]))
        copies[-1].start()

    for (other, chunks), packed in zip(plan, refs):
        side = (own_half() + other) % 2
        for place, chunk in enumerate(chunks):
            start = (side * local + partner(mine, chunk, local)) * width
            span = pl.ds(pl.multiple_of(start, 128), width)
            piece = packed.at[pl.ds(place * rank, rank)]
            put(piece, new_basis_t.at[:, span], len(work), 0)
            work.append((piece, span))
    for i, (piece, span) in enumerate(work):
        upper, lower = split(piece[...])
        right = jnp.concatenate([upper, upper, lower], axis=0)
        approx = jnp.dot(left, right, preferred_element_type=F32)
        merged = g[:, span].astype(F32) + f[:, span].astype(F32)
        staged[i] = (merged - approx).astype(BF16)
        put(staged.at[i], feedback.at[:, span], i, 1)
    for copy in copies:
        copy.wait()


def body(gradient, feedback, basis_in):
    g, f = gradient[0], feedback[0]
    rows, columns = g.shape
    b = basis_in.T
    rank = b.shape[0]
    local, dp = lax.axis_size("local"), lax.axis_size("dp")
    groups = dp // 2
    half = columns // 2
    width = half // local

    def permute(value, along_local, step, cross=None):
        pairs = []
        for x in range(local):
            for z in range(groups):
                to = (partner(x, step, local), z) if along_local else (x, partner(z, step, groups))
                flip = odd_bits(step, local if along_local else groups) if cross is None else cross
                for core in range(2):
                    pairs.append((x * dp + 2 * z + core, to[0] * dp + 2 * to[1] + (core ^ flip)))
        if partner(0, step, local if along_local else groups) != step:
            pairs = [(to, source) for source, to in pairs]
        return lax.ppermute(value, AXES, pairs)

    def swap(value):
        return lax.ppermute(value, AXES, [(i, i ^ 1) for i in range(local * dp)])

    def total_over(value, along_local, direct=False, cross=None, turn=0):
        size = local if along_local else groups
        double = not direct and not size & (size - 1)
        first = value
        steps = [1 << i for i in range(size.bit_length() - 1)] if double else range(1, size)
        for step in steps[::-1] if turn else steps:
            other = permute(value if double else first, along_local, step, cross)
            value = value + other
        return value

    def gather(own, turn):
        if local & (local - 1):
            return [own] + [permute(own, True, s) for s in range(1, local)]
        blocks = {0: own}
        steps = [1 << i for i in range(local.bit_length() - 1)]
        for step in steps[::-1] if turn else steps:
            new = {}
            for place, block in blocks.items():
                new[place ^ step] = permute(block, True, step)
            blocks.update(new)
        return [blocks[place] for place in range(local)]

    g, f, send = call(
        load_kernel,
        [(g.shape, g.dtype), (f.shape, f.dtype), ((rows, half), F32)],
        *(pltpu.with_memory_space_constraint(x, pltpu.HBM) for x in (g, f)),
        scratch=[pltpu.SemaphoreType.DMA((2,))], space=pltpu.HBM,
    )
    left = call(left_kernel, ((rank, rows), F32), g, f, b, flops=1 << 27)
    got = swap(send)
    left = total_over(left, True, direct=True, cross=1)
    chunks = call(pair_kernel, [((rows, width), F32)] * local, g, f, got)
    terms = [chunks[0]] + [permute(chunks[s], True, s) for s in range(1, local)]
    left = total_over(left, False, cross=1)
    basis, basis_t = call(
        functools.partial(gram_schmidt_kernel, 4),
        [((rows, rank), F32), ((rank, rows), F32)],
        left, swap(left), flops=1 << 26,
    )
    rights = call(right_kernel, [((rank // PARTS, width), F32)] * PARTS, basis_t, *terms, flops=1 << 25)
    gathered = []
    for part, right in enumerate(rights):
        total = total_over(right, False, turn=part % 2)
        gathered.append(gather(total, part % 2))
    groups_of = [chunks for chunks in (tuple(range(local - 1)), (local - 1,)) if chunks]
    own, others = [], []
    for chunks in groups_of:
        pieces = [blocks[chunk] for chunk in chunks for blocks in gathered]
        own.append(call(pack_kernel, ((len(chunks) * rank, width), F32), *pieces))
        others.append(swap(own[-1]))
    early, late = groups_of[0], groups_of[-1]
    stages = [((0, early, own[0]),), ((1, late, others[-1]),)]
    if len(groups_of) > 1:
        stages.insert(1, ((1, early, others[0]), (0, late, own[-1])))
    outs = ()
    for stage in stages:
        count = sum(len(chunks) for _, chunks, _ in stage)
        outs = call(
            functools.partial(final_kernel, local * dp, [(other, chunks) for other, chunks, _ in stage]),
            [((rows, columns), BF16), ((rank, columns), F32)],
            g, f, basis, *[packed for _, _, packed in stage], *outs,
            flops=1 << 27, aliased=len(outs), target=pltpu.HBM,
            scratch=[VMEM((count, rows, width), BF16), pltpu.SemaphoreType.DMA((count, 2))],
        )
    return (outs[0][None], outs[1].T)


def solution(mesh):
    return jax.shard_map(
        body,
        mesh=mesh,
        in_specs=(P(("local", "dp"), None, None), P(("local", "dp"), None, None), P()),
        out_specs=(P(("local", "dp"), None, None), P()),
        check_vma=False,
    )
```

```python
import functools

import jax
import jax.numpy as jnp
from jax import lax
from jax.experimental import pallas as pl
from jax.experimental.pallas import tpu as pltpu
from jax.sharding import PartitionSpec as P


epsilon = 1e-06
AXES = ("local", "dp")
F32, BF16 = jnp.float32, jnp.bfloat16
VMEM = pltpu.VMEM
PARTS = 2


def call(kernel, outs, *args, flops=1 << 20, limit=12, scratch=(), space=VMEM, target=VMEM, aliased=0):
    many = isinstance(outs, list)
    shapes = [jax.ShapeDtypeStruct(s, d) for s, d in (outs if many else [outs])]
    size = sum(a.size * a.dtype.itemsize for a in args)
    plain = len(args) - aliased
    result = pl.pallas_call(
        kernel,
        out_shape=shapes,
        in_specs=[pl.BlockSpec(memory_space=space)] * plain + [pl.BlockSpec(memory_space=target)] * aliased,
        out_specs=[pl.BlockSpec(memory_space=target)] * len(shapes),
        input_output_aliases={plain + i: i for i in range(aliased)},
        scratch_shapes=scratch,
        compiler_params=pltpu.CompilerParams(vmem_limit_bytes=limit << 20),
        cost_estimate=pl.CostEstimate(flops=flops, bytes_accessed=size, transcendentals=0),
    )(*args)
    return result if many else result[0]


def split(value):
    high = value.astype(BF16)
    return high, (value - high.astype(F32)).astype(BF16)


def partner(index, step, size):
    if size & (size - 1):
        return (index + step) % size
    return index ^ step


def odd_bits(index, size):
    total = 0
    while size > 1 and not size & (size - 1):
        total, index, size = total + index % 2, index // 2, size // 2
    return total % 2


def own_half():
    local, dp = lax.axis_size("local"), lax.axis_size("dp")
    place = lax.axis_index("dp")
    return (place % 2 + odd_bits(lax.axis_index("local"), local) + odd_bits(place // 2, dp // 2)) % 2


def load_kernel(g, f, gv, fv, send, sems):
    copies = [pltpu.make_async_copy(x, y, sems.at[i]) for i, (x, y) in enumerate(((g, gv), (f, fv)))]
    for copy in copies:
        copy.start()
    for copy in copies:
        copy.wait()
    width = send.shape[1]
    half = own_half()
    for side in range(2):

        @pl.when(half == 1 - side)
        def _():
            span = slice(side * width, (side + 1) * width)
            send[...] = gv[:, span].astype(F32) + fv[:, span].astype(F32)


def left_kernel(g, f, b, left):
    rank = b.shape[0]
    high, low = split(b[...])
    basis = jnp.concatenate([high, low], axis=0)
    dims = (((1,), (1,)), ((), ()))
    both = lax.dot_general(basis, g[...], dims, preferred_element_type=F32)
    both += lax.dot_general(basis, f[...], dims, preferred_element_type=F32)
    left[...] = both[:rank] + both[rank:]


def pair_kernel(g, f, got, *outs):
    width = outs[0].shape[1]
    mine = lax.axis_index("local")
    start = own_half() * got.shape[1]
    for step, out in enumerate(outs):
        inner = pl.multiple_of(partner(mine, step, len(outs)) * width, 128)
        span = pl.ds(pl.multiple_of(start + inner, 128), width)
        out[...] = g[:, span].astype(F32) + f[:, span].astype(F32) + got[:, pl.ds(inner, width)]


def column_sum(value):
    rows = value.shape[0]
    if rows % 8:
        return jnp.sum(value, axis=0, keepdims=True)
    terms = [value[i : i + 8] for i in range(0, rows, 8)]
    while len(terms) > 1:
        terms = [sum(terms[i + 1 : i + 2], terms[i]) for i in range(0, len(terms), 2)]
    return jnp.sum(terms[0], axis=0, keepdims=True)


def gram_schmidt_kernel(window, a, b, basis, basis_t):
    rank, rows = a.shape
    lanes = 128
    total = jnp.concatenate([a[...] + b[...], jnp.zeros((lanes - rank, rows), F32)], axis=0)
    work = total.T
    lane = lax.broadcasted_iota(jnp.int32, (1, lanes), 1)

    def spread(index):
        return jnp.broadcast_to(work[:, index : index + 1], (rows, lanes))

    columns = {index: spread(index) for index in range(min(window, rank))}
    for index in range(rank):
        column = columns.pop(index)
        scale = lax.rsqrt(column_sum(column * column) + epsilon)
        unit = column * scale
        for later in columns:
            columns[later] = columns[later] - unit * (column_sum(column * columns[later]) * scale)
        dots = jnp.where(lane > index, column_sum(column * work) * scale, 0.0)
        work = jnp.where(lane == index, unit, work - unit * dots)
        if index + window < rank:
            columns[index + window] = spread(index + window)
    basis[...] = work[:, :rank]
    basis_t[...] = work.T[:rank]


def right_kernel(basis_t, *refs):
    terms, outs = refs[:-PARTS], refs[-PARTS:]
    total = terms[0][...]
    for term in terms[1:]:
        total = total + term[...]
    both = jnp.dot(basis_t[...], total, precision=lax.Precision.HIGHEST, preferred_element_type=F32)
    size = outs[0].shape[0]
    for i, out in enumerate(outs):
        out[...] = both[i * size : (i + 1) * size]


def pack_kernel(*refs):
    *blocks, out = refs
    size = blocks[0].shape[0]
    for i, block in enumerate(blocks):
        out[i * size : (i + 1) * size] = block[...]


def final_kernel(workers, plan, g, f, basis, *refs):
    feedback, new_basis_t, staged, sems = refs[-4:]
    rank = basis.shape[1]
    width = refs[0].shape[1]
    local = lax.axis_size("local")
    mine = lax.axis_index("local")
    high, low = split(basis[...] * (1.0 / workers))
    left = jnp.concatenate([high, low, high], axis=1)
    work, copies = [], []

    def put(source, target, i, j):
        copies.append(pltpu.make_async_copy(source, target, sems.at[i, j]))
        copies[-1].start()

    for (other, chunks), packed in zip(plan, refs):
        side = (own_half() + other) % 2
        for place, chunk in enumerate(chunks):
            start = (side * local + partner(mine, chunk, local)) * width
            span = pl.ds(pl.multiple_of(start, 128), width)
            piece = packed.at[pl.ds(place * rank, rank)]
            put(piece, new_basis_t.at[:, span], len(work), 0)
            work.append((piece, span))
    for i, (piece, span) in enumerate(work):
        upper, lower = split(piece[...])
        right = jnp.concatenate([upper, upper, lower], axis=0)
        approx = jnp.dot(left, right, preferred_element_type=F32)
        merged = g[:, span].astype(F32) + f[:, span].astype(F32)
        staged[i] = (merged - approx).astype(BF16)
        put(staged.at[i], feedback.at[:, span], i, 1)
    for copy in copies:
        copy.wait()


def body(gradient, feedback, basis_in):
    g, f = gradient[0], feedback[0]
    rows, columns = g.shape
    b = basis_in.T
    rank = b.shape[0]
    local, dp = lax.axis_size("local"), lax.axis_size("dp")
    groups = dp // 2
    half = columns // 2
    width = half // local

    def permute(value, along_local, step, cross=None):
        pairs = []
        for x in range(local):
            for z in range(groups):
                to = (partner(x, step, local), z) if along_local else (x, partner(z, step, groups))
                flip = odd_bits(step, local if along_local else groups) if cross is None else cross
                for core in range(2):
                    pairs.append((x * dp + 2 * z + core, to[0] * dp + 2 * to[1] + (core ^ flip)))
        if partner(0, step, local if along_local else groups) != step:
            pairs = [(to, source) for source, to in pairs]
        return lax.ppermute(value, AXES, pairs)

    def swap(value):
        return lax.ppermute(value, AXES, [(i, i ^ 1) for i in range(local * dp)])

    def total_over(value, along_local, direct=False, cross=None, turn=0, only=None):
        size = local if along_local else groups
        double = not (direct and size <= 4) and not size & (size - 1)
        first = value
        steps = doubling(size) if double else range(1, size)
        if only is not None:
            steps = only
        for step in steps[::-1] if turn else steps:
            other = permute(value if double else first, along_local, step, cross)
            value = value + other
        return value

    def doubling(size):
        return [] if size & (size - 1) else [1 << i for i in range(size.bit_length() - 1)]

    def gather(own, turn):
        if local & (local - 1):
            return [own] + [permute(own, True, s) for s in range(1, local)]
        blocks = {0: own}
        steps = [1 << i for i in range(local.bit_length() - 1)]
        for step in steps[::-1] if turn else steps:
            new = {}
            for place, block in blocks.items():
                new[place ^ step] = permute(block, True, step)
            blocks.update(new)
        return [blocks[place] for place in range(local)]

    g, f, send = call(
        load_kernel,
        [(g.shape, g.dtype), (f.shape, f.dtype), ((rows, half), F32)],
        *(pltpu.with_memory_space_constraint(x, pltpu.HBM) for x in (g, f)),
        scratch=[pltpu.SemaphoreType.DMA((2,))], space=pltpu.HBM,
    )
    left = call(left_kernel, ((rank, rows), F32), g, f, b, flops=1 << 27)
    got = swap(send)
    near = doubling(groups)[:1] or None
    left = total_over(left, False, cross=1, only=near)
    other = swap(left)
    left = left + other
    left = total_over(left, True, direct=True, cross=1)
    chunks = call(pair_kernel, [((rows, width), F32)] * local, g, f, got)
    terms = [chunks[0]] + [permute(chunks[s], True, s) for s in range(1, local)]
    far = doubling(groups)[1:]
    left = total_over(left, False, cross=1, only=far[:-1])
    other = permute(left, False, far[-1], 1) if far else jnp.zeros_like(left)
    basis, basis_t = call(
        functools.partial(gram_schmidt_kernel, 4),
        [((rows, rank), F32), ((rank, rows), F32)],
        left, other, flops=1 << 26,
    )
    rights = call(right_kernel, [((rank // PARTS, width), F32)] * PARTS, basis_t, *terms, flops=1 << 25)
    gathered = []
    for part, right in enumerate(rights):
        total = total_over(right, False, turn=part % 2)
        gathered.append(gather(total, part % 2))
    groups_of = [chunks for chunks in (tuple(range(local - 1)), (local - 1,)) if chunks]
    own, others = [], []
    for chunks in groups_of:
        pieces = [blocks[chunk] for chunk in chunks for blocks in gathered]
        own.append(call(pack_kernel, ((len(chunks) * rank, width), F32), *pieces))
        others.append(swap(own[-1]))
    early, late = groups_of[0], groups_of[-1]
    stages = [((0, early, own[0]),), ((1, late, others[-1]),)]
    if len(groups_of) > 1:
        stages.insert(1, ((1, early, others[0]), (0, late, own[-1])))
    outs = ()
    for stage in stages:
        count = sum(len(chunks) for _, chunks, _ in stage)
        outs = call(
            functools.partial(final_kernel, local * dp, [(other, chunks) for other, chunks, _ in stage]),
            [((rows, columns), BF16), ((rank, columns), F32)],
            g, f, basis, *[packed for _, _, packed in stage], *outs,
            flops=1 << 27, aliased=len(outs), target=pltpu.HBM,
            scratch=[VMEM((count, rows, width), BF16), pltpu.SemaphoreType.DMA((count, 2))],
        )
    return (outs[0][None], outs[1].T)


def solution(mesh):
    return jax.shard_map(
        body,
        mesh=mesh,
        in_specs=(P(("local", "dp"), None, None), P(("local", "dp"), None, None), P()),
        out_specs=(P(("local", "dp"), None, None), P()),
        check_vma=False,
    )
```

```python
import functools

import jax
import jax.numpy as jnp
from jax import lax
from jax.experimental import pallas as pl
from jax.experimental.pallas import tpu as pltpu
from jax.sharding import PartitionSpec as P


epsilon = 1e-06
AXES = ("local", "dp")
F32, BF16 = jnp.float32, jnp.bfloat16
VMEM = pltpu.VMEM
PARTS = 2


def call(kernel, outs, *args, flops=1 << 20, limit=12, scratch=(), space=VMEM, target=VMEM, aliased=0):
    many = isinstance(outs, list)
    shapes = [jax.ShapeDtypeStruct(s, d) for s, d in (outs if many else [outs])]
    size = sum(a.size * a.dtype.itemsize for a in args)
    plain = len(args) - aliased
    result = pl.pallas_call(
        kernel,
        out_shape=shapes,
        in_specs=[pl.BlockSpec(memory_space=space)] * plain + [pl.BlockSpec(memory_space=target)] * aliased,
        out_specs=[pl.BlockSpec(memory_space=target)] * len(shapes),
        input_output_aliases={plain + i: i for i in range(aliased)},
        scratch_shapes=scratch,
        compiler_params=pltpu.CompilerParams(vmem_limit_bytes=limit << 20),
        cost_estimate=pl.CostEstimate(flops=flops, bytes_accessed=size, transcendentals=0),
    )(*args)
    return result if many else result[0]


def split(value):
    high = value.astype(BF16)
    return high, (value - high.astype(F32)).astype(BF16)


def partner(index, step, size):
    if size & (size - 1):
        return (index + step) % size
    return index ^ step


def odd_bits(index, size):
    total = 0
    while size > 1 and not size & (size - 1):
        total, index, size = total + index % 2, index // 2, size // 2
    return total % 2


def own_half():
    local, dp = lax.axis_size("local"), lax.axis_size("dp")
    place = lax.axis_index("dp")
    return (place % 2 + odd_bits(lax.axis_index("local"), local) + odd_bits(place // 2, dp // 2)) % 2


def load_kernel(g, f, gv, fv, send, sems):
    width = send.shape[1]
    half = own_half()
    copies = []
    for side in range(2):
        span = pl.ds(pl.multiple_of((half + 1 + side) % 2 * width, 128), width)
        for i, (x, y) in enumerate(((g, gv), (f, fv))):
            copies.append(pltpu.make_async_copy(x.at[:, span], y.at[:, span], sems.at[side, i]))
            copies[-1].start()
    for copy in copies[:2]:
        copy.wait()
    for side in range(2):

        @pl.when(half == 1 - side)
        def _():
            span = slice(side * width, (side + 1) * width)
            send[...] = gv[:, span].astype(F32) + fv[:, span].astype(F32)

    for copy in copies[2:]:
        copy.wait()


def left_kernel(g, f, b, left):
    rank = b.shape[0]
    high, low = split(b[...])
    basis = jnp.concatenate([high, low], axis=0)
    dims = (((1,), (1,)), ((), ()))
    both = lax.dot_general(basis, g[...], dims, preferred_element_type=F32)
    both += lax.dot_general(basis, f[...], dims, preferred_element_type=F32)
    left[...] = both[:rank] + both[rank:]


def pair_kernel(g, f, got, *outs):
    width = outs[0].shape[1]
    mine = lax.axis_index("local")
    start = own_half() * got.shape[1]
    for step, out in enumerate(outs):
        inner = pl.multiple_of(partner(mine, step, len(outs)) * width, 128)
        span = pl.ds(pl.multiple_of(start + inner, 128), width)
        out[...] = g[:, span].astype(F32) + f[:, span].astype(F32) + got[:, pl.ds(inner, width)]


def column_sum(value):
    rows = value.shape[0]
    if rows % 8:
        return jnp.sum(value, axis=0, keepdims=True)
    terms = [value[i : i + 8] for i in range(0, rows, 8)]
    while len(terms) > 1:
        terms = [sum(terms[i + 1 : i + 2], terms[i]) for i in range(0, len(terms), 2)]
    return jnp.sum(terms[0], axis=0, keepdims=True)


def gram_schmidt_kernel(window, a, b, basis, basis_t):
    rank, rows = a.shape
    lanes = 128
    total = jnp.concatenate([a[...] + b[...], jnp.zeros((lanes - rank, rows), F32)], axis=0)
    work = total.T
    lane = lax.broadcasted_iota(jnp.int32, (1, lanes), 1)

    def spread(index):
        return jnp.broadcast_to(work[:, index : index + 1], (rows, lanes))

    columns = {index: spread(index) for index in range(min(window, rank))}
    for index in range(rank):
        column = columns.pop(index)
        scale = lax.rsqrt(column_sum(column * column) + epsilon)
        unit = column * scale
        for later in columns:
            columns[later] = columns[later] - unit * (column_sum(column * columns[later]) * scale)
        dots = jnp.where(lane > index, column_sum(column * work) * scale, 0.0)
        work = jnp.where(lane == index, unit, work - unit * dots)
        if index + window < rank:
            columns[index + window] = spread(index + window)
    basis[...] = work[:, :rank]
    basis_t[...] = work.T[:rank]


def right_kernel(basis_t, *refs):
    terms, outs = refs[:-PARTS], refs[-PARTS:]
    total = terms[0][...]
    for term in terms[1:]:
        total = total + term[...]
    high, low = split(basis_t[...])
    upper, lower = split(total)
    left = jnp.concatenate([high, low, high], axis=1)
    right = jnp.concatenate([upper, upper, lower], axis=0)
    both = jnp.dot(left, right, preferred_element_type=F32)
    size = outs[0].shape[0]
    for i, out in enumerate(outs):
        out[...] = both[i * size : (i + 1) * size]


def pack_kernel(*refs):
    *blocks, out = refs
    size = blocks[0].shape[0]
    for i, block in enumerate(blocks):
        out[i * size : (i + 1) * size] = block[...]


def final_kernel(workers, plan, g, f, basis, *refs):
    feedback, new_basis_t, staged, sems = refs[-4:]
    rank = basis.shape[1]
    width = refs[0].shape[1]
    local = lax.axis_size("local")
    mine = lax.axis_index("local")
    high, low = split(basis[...] * (1.0 / workers))
    left = jnp.concatenate([high, low, high], axis=1)
    work, copies = [], []

    def put(source, target, i, j):
        copies.append(pltpu.make_async_copy(source, target, sems.at[i, j]))
        copies[-1].start()

    for (other, chunks), packed in zip(plan, refs):
        side = (own_half() + other) % 2
        for place, chunk in enumerate(chunks):
            start = (side * local + partner(mine, chunk, local)) * width
            span = pl.ds(pl.multiple_of(start, 128), width)
            piece = packed.at[pl.ds(place * rank, rank)]
            put(piece, new_basis_t.at[:, span], len(work), 0)
            work.append((piece, span))
    for i, (piece, span) in enumerate(work):
        upper, lower = split(piece[...])
        right = jnp.concatenate([upper, upper, lower], axis=0)
        approx = jnp.dot(left, right, preferred_element_type=F32)
        merged = g[:, span].astype(F32) + f[:, span].astype(F32)
        staged[i] = (merged - approx).astype(BF16)
        put(staged.at[i], feedback.at[:, span], i, 1)
    for copy in copies:
        copy.wait()


def body(gradient, feedback, basis_in):
    g, f = gradient[0], feedback[0]
    rows, columns = g.shape
    b = basis_in.T
    rank = b.shape[0]
    local, dp = lax.axis_size("local"), lax.axis_size("dp")
    groups = dp // 2
    half = columns // 2
    width = half // local

    def permute(value, along_local, step, cross=None):
        pairs = []
        for x in range(local):
            for z in range(groups):
                to = (partner(x, step, local), z) if along_local else (x, partner(z, step, groups))
                flip = odd_bits(step, local if along_local else groups) if cross is None else cross
                for core in range(2):
                    pairs.append((x * dp + 2 * z + core, to[0] * dp + 2 * to[1] + (core ^ flip)))
        if partner(0, step, local if along_local else groups) != step:
            pairs = [(to, source) for source, to in pairs]
        return lax.ppermute(value, AXES, pairs)

    def swap(value):
        return lax.ppermute(value, AXES, [(i, i ^ 1) for i in range(local * dp)])

    def total_over(value, along_local, direct=False, cross=None, turn=0, only=None):
        size = local if along_local else groups
        double = not (direct and size <= 4) and not size & (size - 1)
        first = value
        steps = doubling(size) if double else range(1, size)
        if only is not None:
            steps = only
        for step in steps[::-1] if turn else steps:
            other = permute(value if double else first, along_local, step, cross)
            value = value + other
        return value

    def doubling(size):
        return [] if size & (size - 1) else [1 << i for i in range(size.bit_length() - 1)]

    def gather(own, turn):
        if local & (local - 1):
            return [own] + [permute(own, True, s) for s in range(1, local)]
        blocks = {0: own}
        steps = [1 << i for i in range(local.bit_length() - 1)]
        for step in steps[::-1] if turn else steps:
            new = {}
            for place, block in blocks.items():
                new[place ^ step] = permute(block, True, step)
            blocks.update(new)
        return [blocks[place] for place in range(local)]

    g, f, send = call(
        load_kernel,
        [(g.shape, g.dtype), (f.shape, f.dtype), ((rows, half), F32)],
        *(pltpu.with_memory_space_constraint(x, pltpu.HBM) for x in (g, f)),
        scratch=[pltpu.SemaphoreType.DMA((2, 2))], space=pltpu.HBM,
    )
    left = call(left_kernel, ((rank, rows), F32), g, f, b, flops=1 << 27)
    got = swap(send)
    near = doubling(groups)[:1] or None
    left = total_over(left, False, cross=1, only=near)
    other = swap(left)
    left = left + other
    left = total_over(left, True, direct=True, cross=1)
    chunks = call(pair_kernel, [((rows, width), F32)] * local, g, f, got)
    terms = [chunks[0]] + [permute(chunks[s], True, s) for s in range(1, local)]
    far = doubling(groups)[1:]
    left = total_over(left, False, cross=1, only=far[:-1])
    other = permute(left, False, far[-1], 1) if far else jnp.zeros_like(left)
    basis, basis_t = call(
        functools.partial(gram_schmidt_kernel, 4),
        [((rows, rank), F32), ((rank, rows), F32)],
        left, other, flops=1 << 26,
    )
    rights = call(right_kernel, [((rank // PARTS, width), F32)] * PARTS, basis_t, *terms, flops=1 << 25)
    gathered = []
    for part, right in enumerate(rights):
        total = total_over(right, False, turn=part % 2)
        gathered.append(gather(total, part % 2))
    groups_of = [chunks for chunks in (tuple(range(local - 1)), (local - 1,)) if chunks]
    own, others = [], []
    for chunks in groups_of:
        pieces = [blocks[chunk] for chunk in chunks for blocks in gathered]
        own.append(call(pack_kernel, ((len(chunks) * rank, width), F32), *pieces))
        others.append(swap(own[-1]))
    early, late = groups_of[0], groups_of[-1]
    stages = [((0, early, own[0]),), ((1, late, others[-1]),)]
    if len(groups_of) > 1:
        stages.insert(1, ((1, early, others[0]), (0, late, own[-1])))
    outs = ()
    for stage in stages:
        count = sum(len(chunks) for _, chunks, _ in stage)
        outs = call(
            functools.partial(final_kernel, local * dp, [(other, chunks) for other, chunks, _ in stage]),
            [((rows, columns), BF16), ((rank, columns), F32)],
            g, f, basis, *[packed for _, _, packed in stage], *outs,
            flops=1 << 27, aliased=len(outs), target=pltpu.HBM,
            scratch=[VMEM((count, rows, width), BF16), pltpu.SemaphoreType.DMA((count, 2))],
        )
    return (outs[0][None], outs[1].T)


def solution(mesh):
    return jax.shard_map(
        body,
        mesh=mesh,
        in_specs=(P(("local", "dp"), None, None), P(("local", "dp"), None, None), P()),
        out_specs=(P(("local", "dp"), None, None), P()),
        check_vma=False,
    )
```
